256 devices in a mesh: grp: 16 (over x_lo, y, core), sp: 16 (over z, x_hi).
Axes of the slice: x: 4 (x_hi: 2, x_lo: 2; x = x_hi * 2 + x_lo), y: 4, z: 8, core: 2. Of those that a mesh axis runs over, the one named last changes fastest.
Arguments:
- latents: bfloat16 [16, 2048, 3072], P('grp', 'sp'), may hold values from -6 to 6
- timestep: int32 [16], P('grp'), may hold values from 0 to 999
- w_mod: bfloat16 [256, 9216], replicated, may hold values from -0.375 to 0.375
- w_qkv: bfloat16 [16, 3072, 384], P('sp', 'grp'), may hold values from -2 to 2
- w_out: bfloat16 [16, 128, 3072], P('sp', 'grp'), may hold values from -0.5 to 0.5
Outputs:
- update: bfloat16 [16, 2048, 3072], P('grp', 'sp')
The draws below stay inside these ranges and needn't reach their ends.
All inputs are finite; a program needn't handle non-finite values.
Results may differ from the reference program's by a relative error of at most 0.012.
Values may be sent and summed in bfloat16 or wider, within the bound.
A program may use at most 128 MiB of HBM per device.

```python
import math
import jax
import jax.numpy as jnp
from jax import lax

D = 3072
HS = 128
FREQ = 256
H = 16
LEN = 2048
IMAGES = 16


def draw_w_qkv(key, part):
    first, second, third = jax.random.split(jax.random.fold_in(key, 17), 3)
    base = 1.0 / math.sqrt(D)
    query_part = jax.random.normal(first, (H, D, HS), jnp.float32) * (1.5 * base)
    value_part = jax.random.normal(third, (H, D, HS), jnp.float32) * base
    key_part = jax.random.normal(second, (H, D, HS), jnp.float32) * base
    whole = jnp.concatenate([query_part, key_part, value_part], axis=2)
    return jnp.clip(whole, -2.0, 2.0).astype(jnp.bfloat16)


def plant(array, stream_key, smallest, top_value):
    spot = [jax.random.randint(jax.random.fold_in(stream_key, axis), (), 0, length) for axis, length in enumerate(array.shape)]
    main_axis = array.shape.index(max(array.shape))
    next_to = spot[:main_axis] + [(spot[main_axis] + 1) % array.shape[main_axis]] + spot[main_axis + 1:]
    return array.at[tuple(spot)].set(smallest).at[tuple(next_to)].set(top_value)


def shard_levels(rng, shape, cuts, low, high):
    level, own = 1.0, jax.random.fold_in(rng, 6)
    for dim, shards_of in cuts:
        steps = jnp.exp(jax.random.uniform(jax.random.fold_in(own, dim), (shards_of,), jnp.float32, low / len(cuts), high / len(cuts)))
        level = level * jnp.repeat(steps, shape[dim] // shards_of).reshape([-1 if axis == dim else 1 for axis in range(len(shape))])
    return level


def centred(stream_key, shape, scale, limit, cuts=(), held_as=jnp.bfloat16):
    array = jax.random.normal(stream_key, shape, jnp.float32) * scale
    if len(cuts) > 0:
        array = shard_levels(stream_key, shape, cuts, -0.22, 0.18) * array
    return jnp.clip(array, min=-limit, max=limit).astype(held_as)


def setup_inputs(seed: int = 0) -> dict:
    arg_keys = jax.random.split(jax.random.key(seed), 6)
    latents = centred(arg_keys[0], (IMAGES, LEN, D), 1.0, 6.0, ((0, 16), (1, 16)))
    timestep = plant(jax.random.randint(arg_keys[1], (IMAGES,), 0, 1000), jax.random.fold_in(arg_keys[1], 1), 0, 999).astype(jnp.int32)
    w_mod = centred(arg_keys[2], (FREQ, 3 * D), FREQ ** -0.5, 0.375)
    w_qkv = draw_w_qkv(jax.random.fold_in(arg_keys[5], 71), 0)
    w_out = centred(arg_keys[4], (H, HS, D), HS ** -0.5, 0.5, ((0, 16), (1, 16)))
    return {"latents": latents, "timestep": timestep, "w_mod": w_mod, "w_qkv": w_qkv, "w_out": w_out}


def modulation(timestep, w_mod):
    half_freq = w_mod.shape[0] // 2
    freqs = jnp.exp(-math.log(10000.0) * jnp.arange(half_freq, dtype=jnp.float32) / half_freq)
    angles = timestep.astype(jnp.float32)[:, None] * freqs[None, :]
    embed = jnp.concatenate([jnp.cos(angles), jnp.sin(angles)], axis=1).astype(jnp.bfloat16)
    return jnp.dot(embed, w_mod, preferred_element_type=jnp.float32)

def normalize(latents, shift, scale):
    values = latents.astype(jnp.float32)
    center = lax.optimization_barrier(jnp.mean(values, axis=-1, keepdims=True))
    spread = lax.optimization_barrier(jnp.mean((values - center) ** 2, axis=-1, keepdims=True))
    normed = (values - center) * lax.rsqrt(spread + 1e-06)
    return (normed * (1.0 + scale[:, None, :]) + shift[:, None, :]).astype(jnp.bfloat16)

def attend(query, keys, values):
    length, head_size = query.shape
    block = min(512, length)
    blocks = query.reshape(length // block, block, head_size)

    def one_block(query_rows):
        scores = lax.dot_general(query_rows, keys, (((1,), (1,)), ((), ())), preferred_element_type=jnp.float32)
        scores = scores / math.sqrt(head_size)
        largest = lax.optimization_barrier(jnp.max(scores, axis=1, keepdims=True))
        weights = jnp.exp(scores - largest)
        probs = (weights / lax.optimization_barrier(jnp.sum(weights, axis=1, keepdims=True))).astype(jnp.bfloat16)
        return jnp.dot(probs, values, preferred_element_type=jnp.float32).astype(jnp.bfloat16)
    return lax.map(one_block, blocks).reshape(length, head_size)

def reference(latents, timestep, w_mod, w_qkv, w_out):
    width = latents.shape[2]
    head_size = w_out.shape[1]
    mod = modulation(timestep, w_mod)
    shift = mod[:, :width]
    scale = mod[:, width:2 * width]
    gate = mod[:, 2 * width:]
    normed = normalize(latents, shift, scale)

    def one_image(inputs):
        normed_one, gate_one = inputs

        def one_head(total, weights):
            weight_in, weight_out = weights
            qkv = jnp.dot(normed_one, weight_in, preferred_element_type=jnp.float32).astype(jnp.bfloat16)
            attended = attend(qkv[:, :head_size], qkv[:, head_size:2 * head_size], qkv[:, 2 * head_size:])
            contrib = jnp.dot(attended, weight_out, preferred_element_type=jnp.float32).astype(jnp.bfloat16)
            contrib = lax.optimization_barrier(contrib)
            return (total + contrib.astype(jnp.float32), None)
        start_total = jnp.zeros((normed_one.shape[0], width), jnp.float32)
        total, unused = lax.scan(one_head, start_total, (w_qkv, w_out))
        return (gate_one[None, :] * total).astype(jnp.bfloat16)
    return lax.map(one_image, (normed, gate))
```

```python
import functools
import math

import jax
import jax.numpy as jnp
from jax import lax
from jax.experimental import pallas as pl
from jax.experimental.pallas import tpu as pltpu
from jax.sharding import PartitionSpec as P

MESH = pl.DeviceIdType.MESH
BF = jnp.bfloat16
F32 = jnp.float32

TR, TL, WX, WY, WD, OP, OZ, O1A, O1B, O2A, O2B, OD, KX, AZ, COUNT = (
    0, 7, 14, 18, 22, 26, 27, 35, 39, 43, 47, 51, 53, 61, 69,
)


def kernel(embed, lat_hbm, wm_hbm, wqkv_hbm, wout_hbm, out_hbm,
           xin, wm, mod, tok, wq, wo, pw_own, pw_par, qs, kv, at, mx, res,
           ss, rs, ls):
    s = lax.axis_index("sp")
    g = lax.axis_index("grp")
    z, xh = lax.div(s, 2), lax.rem(s, 2)
    xl, y, core = lax.div(g, 8), lax.rem(lax.div(g, 2), 4), lax.rem(g, 2)
    x = xh * 2 + xl

    def dev(zz, xx, yy, cc):
        grp = (lax.rem(xx, 2) * 4 + yy) * 2 + cc
        return (grp, zz * 2 + lax.div(xx, 2))

    zpeer = {o: dev(lax.rem(z + o, 8), x, y, core) for o in range(1, 8)}
    xpeer = {o: dev(z, lax.rem(x + o, 4), y, core) for o in range(1, 4)}
    ypeer = {o: dev(z, x, lax.rem(y + o, 4), core) for o in range(1, 4)}
    partner = dev(z, x, y, 1 - core)
    right, left = zpeer[1], zpeer[7]

    def rc(src, dst, i, to):
        return pltpu.make_async_remote_copy(
            src_ref=src, dst_ref=dst, send_sem=ss.at[i], recv_sem=rs.at[i],
            device_id=to, device_id_type=MESH,
        )

    sent = []

    def send(*args):
        copy = rc(*args)
        copy.start()
        sent.append(copy)
        return copy

    cols = pl.ds(pl.multiple_of(xh * 384, 128), 384)
    own_w = wq.at[xl, y, core, :, cols]

    c_w = pltpu.make_async_copy(wqkv_hbm, own_w, ls.at[0])
    c_o = pltpu.make_async_copy(wout_hbm, pw_own, ls.at[1])
    c_x = pltpu.make_async_copy(lat_hbm, xin, ls.at[2])
    c_m = pltpu.make_async_copy(wm_hbm.at[:, pl.ds(0, 6144)], wm.at[:, pl.ds(0, 6144)], ls.at[3])
    c_g = pltpu.make_async_copy(wm_hbm.at[:, pl.ds(6144, 3072)], wm.at[:, pl.ds(6144, 3072)], ls.at[4])
    for c in (c_w, c_o, c_m, c_x, c_g):
        c.start()

    barrier = pltpu.get_barrier_semaphore()
    for p in (*zpeer.values(), *xpeer.values(), *ypeer.values(), partner):
        pl.semaphore_signal(barrier, inc=1, device_id=p, device_id_type=MESH)
    c_w.wait()
    c_o.wait()
    pl.semaphore_wait(barrier, 14)

    wx = [send(own_w, own_w, WX + o, xpeer[o]) for o in (1, 3, 2)]
    op = send(pw_own, pw_par, OP, partner)

    def modulate(lo, hi):
        for j in range(lo, hi):
            mod[j] = jnp.dot(embed[...], wm[:, j * 768:(j + 1) * 768], preferred_element_type=F32)

    c_m.wait()
    modulate(0, 8)
    c_x.wait()

    op.wait_recv()
    first = core == 0
    for j in range(2):
        def half(ref):
            a = ref[:, j * 768:(j + 1) * 768].astype(F32)
            b = ref[:, 1536 + j * 768:1536 + (j + 1) * 768].astype(F32)
            return jnp.where(first, a, b)
        a, b = half(pw_own), half(pw_par)
        rows = jnp.concatenate([jnp.where(first, a, b), jnp.where(first, b, a)], axis=0)
        wo[core * 2 + j, z, xh, xl, y] = rows.astype(BF)
    own_o = wo.at[pl.ds(core * 2, 2), z, xh, xl, y]
    oz = [send(own_o, own_o, OZ + o, zpeer[o]) for o in (4, 3, 5, 2, 6, 1, 7)]

    def norm_rows(i, carry):
        r = pl.ds(pl.multiple_of(i * 16, 16), 16)
        v = xin[r, :].astype(F32)
        center = jnp.sum(v, axis=-1, keepdims=True) * (1.0 / 3072)
        v = v - center
        spread = jnp.sum(v * v, axis=-1, keepdims=True) * (1.0 / 3072)
        v = v * lax.rsqrt(spread + 1e-06)
        for j in range(4):
            c = slice(j * 768, (j + 1) * 768)
            tok[0, r, c] = (v[:, c] * (1.0 + mod[4 + j]) + mod[j]).astype(BF)
        return carry

    part = (pl.ds(0, 64), pl.ds(64, 64))

    def tright(k):
        d, c = k // 2, k % 2
        return send(tok.at[d, part[c]], tok.at[d + 1, part[c]], TR + k, right)

    def tleft(k):
        d, c = k // 2, 1 - k % 2
        return send(tok.at[(8 - d) % 8, part[c]], tok.at[7 - d, part[c]], TL + k, left)

    tr, tl = {}, {}
    lax.fori_loop(0, 4, norm_rows, 0)
    tr[0] = tright(0)
    lax.fori_loop(4, 8, norm_rows, 0)
    tl[0] = tleft(0)
    tr[1] = tright(1)
    tl[1] = tleft(1)

    c_g.wait()
    modulate(8, 12)

    for c in wx:
        c.wait_recv()
    for c in oz:
        c.wait_recv()

    def sub(j):
        return wo.at[core * 2 + j, :, xh, xl, y]

    o1a = [send(sub(0), sub(0), O1A + o, xpeer[o]) for o in (1, 3, 2)]
    o1b = [send(sub(1), sub(1), O1B + o, ypeer[o]) for o in (1, 3, 2)]
    yrow = wq.at[:, y, core]
    wy = {o: send(yrow, yrow, WY + o, ypeer[o]) for o in (1, 3, 2)}
    wd = [send(yrow, yrow, WD, partner)]

    def project(slot):
        acc = jnp.zeros((128, 768), F32)
        for a in range(2):
            w = wq[a].reshape(1536, 768)
            acc += jnp.dot(tok[slot, :, a * 1536:(a + 1) * 1536], w, preferred_element_type=F32)
        acc = acc.astype(BF)
        qs[slot, :, 0:128] = acc[:, 0:128]
        qs[slot, :, 128:256] = acc[:, 384:512]
        kv[slot, :, 0:256] = acc[:, 128:384]
        kv[slot, :, 256:512] = acc[:, 512:768]
        rc(kv.at[slot], kv.at[8 + slot], KX + slot, xpeer[2]).start()

    def project_some(count, slot_of):
        def body(i, carry):
            project(slot_of(i))
            return carry
        lax.fori_loop(0, count, body, 0)

    def od(j):
        ref = wo.at[core * 2 + j]
        return send(ref, ref, OD + j, partner)

    for k in range(7):
        tr[k].wait_recv()
        if k < 5:
            tr[k + 2] = tright(k + 2)
        tl[k].wait_recv()
        if k < 5:
            tl[k + 2] = tleft(k + 2)
        if k == 1:
            for c in o1a:
                c.wait_recv()
            ref = wo.at[core * 2, :, :, :, y]
            o2a = [send(ref, ref, O2A + o, ypeer[o]) for o in (1, 3, 2)]
            for c in o1b:
                c.wait_recv()
            ref = wo.at[core * 2 + 1, :, xh, xl]
            ref1 = wo.at[core * 2 + 1, :, xh, xl]
            o2b = [send(ref, ref1, O2B + o, xpeer[o]) for o in (1, 3, 2)]
        if k == 3:
            for i, o in enumerate((1, 3, 2)):
                wy[o].wait_recv()
                ref = wq.at[:, lax.rem(y + 4 - o, 4), core]
                wd.append(send(ref, ref, WD + o, partner))
            for c in wd:
                c.wait_recv()
            project_some(5, lambda i: lax.rem(i + 6, 8))
        if k == 5:
            project_some(2, lambda i: 3 + 2 * i)
        if k == 6:
            project_some(1, lambda i: i + 4)

    for slot in range(8):
        rc(kv.at[slot], kv.at[8 + slot], KX + slot, xpeer[2]).wait_recv()

    unit = 1.0 / math.sqrt(128)

    def attend(i, carry):
        a, b = 4 + i, 3 - i
        for h in range(2):
            hc = slice(h * 128, (h + 1) * 128)
            q = jnp.concatenate([qs[a, :, hc], qs[b, :, hc]], axis=0)
            keys = kv[:, :, h * 256:h * 256 + 128].reshape(2048, 128)
            vals = kv[:, :, h * 256 + 128:h * 256 + 256].reshape(2048, 128)
            sc = lax.dot_general(q, keys, (((1,), (1,)), ((), ())), preferred_element_type=F32)
            top = jnp.max(sc, axis=1, keepdims=True)
            e = jnp.exp((sc - top) * unit)
            total = jnp.sum(e, axis=1, keepdims=True)
            o = jnp.dot(e.astype(BF), vals, preferred_element_type=F32) / total
            o = o.astype(BF)
            at[a, :, hc] = o[:128]
            at[b, :, hc] = o[128:]
        rc(at.at[a], mx.at[z], AZ + a, dev(lax.rem(z + 8 - a, 8), x, y, core)).start()

        @pl.when(i < 3)
        def _():
            rc(at.at[b], mx.at[z], AZ + b, dev(lax.rem(z + 8 - b, 8), x, y, core)).start()

        return carry

    lax.fori_loop(0, 4, attend, 0)
    mx[z] = at[0]

    for c in o2a:
        c.wait_recv()
    od0 = od(0)
    for c in o2b:
        c.wait_recv()
    od1 = od(1)
    az = [rc(at.at[d], mx.at[z], AZ + d, dev(lax.rem(z + 8 - d, 8), x, y, core)) for d in range(1, 8)]
    for c in az:
        c.wait_recv()

    def out_copy(q):
        return pltpu.make_async_copy(
            res.at[q], out_hbm.at[:, pl.ds(pl.multiple_of(q * 768, 128), 768)], ls.at[q])

    def out_part(i, carry):
        q = lax.rem(core * 2 + i, 4)
        m = jnp.concatenate([mx[k] for k in range(8)], axis=1)
        acc = jnp.dot(m, wo[q].reshape(2048, 768), preferred_element_type=F32)
        res[q] = (acc * mod[8 + q][0:1]).astype(BF)
        out_copy(q).start()
        return carry

    lax.fori_loop(0, 2, out_part, 0)
    od0.wait_recv()
    od1.wait_recv()
    lax.fori_loop(2, 4, out_part, 0)

    for q in range(4):
        out_copy(q).wait()
    for c in sent:
        c.wait_send()
    for slot in range(8):
        rc(kv.at[slot], kv.at[8 + slot], KX + slot, xpeer[2]).wait_send()
    for c in az:
        c.wait_send()


def on_device(latents, timestep, w_mod, w_qkv, w_out):
    half_freq = w_mod.shape[0] // 2
    freqs = jnp.exp(-math.log(10000.0) * jnp.arange(half_freq, dtype=F32) / half_freq)
    angles = timestep.astype(F32)[:, None] * freqs[None, :]
    embed = jnp.concatenate([jnp.cos(angles), jnp.sin(angles)], axis=1).astype(BF)
    embed = jnp.broadcast_to(embed, (16, 2 * half_freq))
    anyspace = pl.BlockSpec(memory_space=pl.ANY)
    out = pl.pallas_call(
        kernel,
        out_shape=jax.ShapeDtypeStruct((128, 3072), BF),
        in_specs=[pl.BlockSpec(memory_space=pltpu.VMEM)] + [anyspace] * 4,
        out_specs=anyspace,
        scratch_shapes=[
            pltpu.VMEM((128, 3072), BF),
            pltpu.VMEM((256, 9216), BF),
            pltpu.VMEM((12, 16, 768), F32),
            pltpu.VMEM((8, 128, 3072), BF),
            pltpu.VMEM((2, 4, 2, 192, 768), BF),
            pltpu.VMEM((4, 8, 2, 2, 4, 16, 768), BF),
            pltpu.VMEM((8, 3072), BF),
            pltpu.VMEM((8, 3072), BF),
            pltpu.VMEM((8, 128, 256), BF),
            pltpu.VMEM((16, 128, 512), BF),
            pltpu.VMEM((8, 128, 256), BF),
            pltpu.VMEM((8, 128, 256), BF),
            pltpu.VMEM((4, 128, 768), BF),
            pltpu.SemaphoreType.DMA((COUNT,)),
            pltpu.SemaphoreType.DMA((COUNT,)),
            pltpu.SemaphoreType.DMA((5,)),
        ],
        compiler_params=pltpu.CompilerParams(
            collective_id=0, has_side_effects=True, vmem_limit_bytes=60 * 1024 * 1024,
        ),
        name="sublayer",
    )(embed, latents[0], w_mod, w_qkv[0], w_out[0])
    return out[None]


def solution(mesh):
    placed = (P("grp", "sp", None), P("grp"), P(), P("sp", "grp", None), P("sp", "grp", None))
    return jax.shard_map(
        on_device, mesh=mesh, in_specs=placed, out_specs=P("grp", "sp", None), check_vma=False
    )
```

```python
import functools
import math

import jax
import jax.numpy as jnp
from jax import lax
from jax.experimental import pallas as pl
from jax.experimental.pallas import tpu as pltpu
from jax.sharding import PartitionSpec as P

MESH = pl.DeviceIdType.MESH
BF = jnp.bfloat16
F32 = jnp.float32

TR, TL, WXA, WYA, WYB, WXB, WD, OP, OZR, OZL = 0, 7, 14, 18, 24, 28, 34, 50, 51, 56
AX, AY, BX, BY, CX, CY, OD, KX, AZ, COUNT = 61, 65, 71, 75, 81, 85, 91, 115, 123, 131

PLACE = (0, 1, 3, 5, 7, 6, 4, 2)


class Direct:
    def __init__(self, send, ref, base, peers):
        self.copies = [send(ref, ref, base + o, peers[o]) for o in (2, 1, 3)]

    def finish(self):
        for c in self.copies:
            c.wait_recv()


class Ring:
    def __init__(self, send, region, me, base, plus, minus, landed=None):
        self.send, self.region, self.base = send, region, base
        self.me, self.plus, self.minus = me, plus, minus
        self.landed = landed
        self.copies = {}
        for k, half, to in ((0, 0, plus), (2, 1, minus), (1, 1, plus), (3, 0, minus)):
            self.go(k, 0, half, to)
        if landed:
            landed(me, 0, 0)
            landed(me, 1, 1)

    def go(self, k, shift, half, to):
        ref = self.region(lax.rem(self.me + shift, 4), half)
        self.copies[k] = self.send(ref, ref, self.base + k, to)

    def arrive(self, k, shift, half, n):
        self.copies[k].wait_recv()
        if self.landed:
            self.landed(lax.rem(self.me + shift, 4), half, n)

    def forward(self):
        self.copies[0].wait_recv()
        self.go(4, 3, 0, self.plus)
        self.copies[2].wait_recv()
        self.go(5, 1, 1, self.minus)
        if self.landed:
            self.landed(lax.rem(self.me + 3, 4), 0, 2)
            self.landed(lax.rem(self.me + 1, 4), 1, 3)

    def near(self):
        self.arrive(1, 3, 1, 4)
        self.arrive(3, 1, 0, 5)

    def far(self):
        self.arrive(4, 2, 0, 6)
        self.arrive(5, 2, 1, 7)

    def finish(self):
        self.near()
        self.far()


def kernel(embed, lat_hbm, wm_hbm, wqkv_hbm, wout_hbm, out_hbm,
           wm, mod, tok, nrm, wq, wo, pw_own, pw_par, qs, kv, at, mx, acc, res,
           ss, rs, ls):
    s = lax.axis_index("sp")
    g = lax.axis_index("grp")
    z, xh = lax.div(s, 2), lax.rem(s, 2)
    xl, y, core = lax.div(g, 8), lax.rem(lax.div(g, 2), 4), lax.rem(g, 2)
    x = xh * 2 + xl

    def dev(zz, xx, yy, cc):
        grp = (lax.rem(xx, 2) * 4 + yy) * 2 + cc
        return (grp, zz * 2 + lax.div(xx, 2))

    zpeer = {o: dev(lax.rem(z + o, 8), x, y, core) for o in range(1, 8)}
    xpeer = {o: dev(z, lax.rem(x + o, 4), y, core) for o in range(1, 4)}
    ypeer = {o: dev(z, x, lax.rem(y + o, 4), core) for o in range(1, 4)}
    partner = dev(z, x, y, 1 - core)
    right, left = zpeer[1], zpeer[7]

    def rc(src, dst, i, to):
        return pltpu.make_async_remote_copy(
            src_ref=src, dst_ref=dst, send_sem=ss.at[i], recv_sem=rs.at[i],
            device_id=to, device_id_type=MESH,
        )

    sent = []

    def send(*args):
        copy = rc(*args)
        copy.start()
        sent.append(copy)
        return copy

    cols = pl.ds(pl.multiple_of(xh * 384, 128), 384)
    own_w = wq.at[xl, y, core, :, cols]

    c_w = pltpu.make_async_copy(wqkv_hbm, own_w, ls.at[0])
    c_o = pltpu.make_async_copy(wout_hbm, pw_own, ls.at[1])
    c_x = pltpu.make_async_copy(lat_hbm, tok.at[0], ls.at[2])
    c_m = pltpu.make_async_copy(wm_hbm, wm, ls.at[3])
    for c in (c_x, c_w, c_o, c_m):
        c.start()

    barrier = pltpu.get_barrier_semaphore()
    for p in (*zpeer.values(), *xpeer.values(), *ypeer.values(), partner):
        pl.semaphore_signal(barrier, inc=1, device_id=p, device_id_type=MESH)
    c_x.wait()
    c_w.wait()
    c_o.wait()
    pl.semaphore_wait(barrier, 14)

    part = (pl.ds(0, 64), pl.ds(64, 64))

    def tright(k):
        d, c = k // 2, k % 2
        return send(tok.at[d, part[c]], tok.at[d + 1, part[c]], TR + k, right)

    def tleft(k):
        d, c = k // 2, 1 - k % 2
        return send(tok.at[(8 - d) % 8, part[c]], tok.at[7 - d, part[c]], TL + k, left)

    tr, tl = {0: tright(0)}, {0: tleft(0)}

    op = send(pw_own, pw_par, OP, partner)
    top, low = pl.ds(0, 96), pl.ds(96, 96)
    wxa = Direct(send, wq.at[xl, y, core, top, cols], WXA, xpeer)
    wyb = Direct(send, wq.at[xl, y, core, low, cols], WYB, ypeer)

    op.wait_recv()
    first = core == 0
    for j in range(2):
        def half(ref):
            a = ref[:, j * 768:(j + 1) * 768].astype(F32)
            b = ref[:, 1536 + j * 768:1536 + (j + 1) * 768].astype(F32)
            return jnp.where(first, a, b)
        a, b = half(pw_own), half(pw_par)
        rows = jnp.concatenate([jnp.where(first, a, b), jnp.where(first, b, a)], axis=0)
        wo[core * 2 + j, 0, xh, xl, y] = rows.astype(BF)

    def slab(slot, far):
        quarter = pl.ds(core * 2, 2) if far is None else core * 2 + far
        return wo.at[quarter, PLACE[slot], xh, xl, y]

    def hop(h):
        r, l = (0, 1) if h == 4 else (None, None)
        return (send(slab(h - 1, r), slab(h, r), OZR + h, right),
                send(slab((9 - h) % 8, l), slab(8 - h, l), OZL + h, left))

    oz = {1: hop(1)}
    tr[1] = tright(1)
    tl[1] = tleft(1)

    c_m.wait()
    for j in range(12):
        mod[j] = jnp.dot(embed[...], wm[:, j * 768:(j + 1) * 768], preferred_element_type=F32)

    def normalize(slot):
        def rows(i, carry):
            r = pl.ds(pl.multiple_of(i * 16, 16), 16)
            v = tok[slot, r, :].astype(F32)
            center = jnp.sum(v, axis=-1, keepdims=True) * (1.0 / 3072)
            v = v - center
            spread = jnp.sum(v * v, axis=-1, keepdims=True) * (1.0 / 3072)
            v = v * lax.rsqrt(spread + 1e-06)
            for j in range(4):
                c = slice(j * 768, (j + 1) * 768)
                nrm[slot, r, c] = (v[:, c] * (1.0 + mod[4 + j]) + mod[j]).astype(BF)
            return carry
        lax.fori_loop(0, 8, rows, 0)

    wd = []

    def wya_region(i, h):
        return wq.at[h, i, core, top]

    def wxb_region(i, h):
        c = pl.ds(pl.multiple_of(lax.div(i, 2) * 384, 128), 384)
        return wq.at[lax.rem(i, 2), pl.ds(h * 2, 2), core, low, c]

    def w_landed(region, base):
        def landed(i, h, n):
            ref = region(i, h)
            wd.append(send(ref, ref, base + n, partner))
        return landed

    wxa.finish()
    wya = Ring(send, wya_region, y, WYA, ypeer[1], ypeer[3], w_landed(wya_region, WD))
    wyb.finish()
    wxb = Ring(send, wxb_region, x, WXB, xpeer[1], xpeer[3], w_landed(wxb_region, WD + 8))
    normalize(0)

    groups = {"a": pl.ds(0, 3), "b": pl.ds(3, 2), "c": pl.ds(5, 3)}
    od = []

    def one(name, base):
        return Direct(send, wo.at[pl.ds(core * 2, 2), groups[name], xh, xl, y], base, xpeer)

    def two(name, base, first_od):
        def region(i, h):
            return wo.at[core * 2 + h, groups[name], :, :, i]

        def landed(i, h, n):
            ref = region(i, h)
            od.append(send(ref, ref, OD + first_od + n, partner))

        return Ring(send, region, y, base, ypeer[1], ypeer[3], landed)

    def project(slot):
        acc = jnp.zeros((128, 768), F32)
        for a in range(2):
            w = wq[a].reshape(1536, 768)
            acc += jnp.dot(nrm[slot, :, a * 1536:(a + 1) * 1536], w, preferred_element_type=F32)
        acc = acc.astype(BF)
        qs[slot, :, 0:128] = acc[:, 0:128]
        qs[slot, :, 128:256] = acc[:, 384:512]
        kv[slot, :, 0:256] = acc[:, 128:384]
        kv[slot, :, 256:512] = acc[:, 512:768]
        rc(kv.at[slot], kv.at[8 + slot], KX + slot, xpeer[2]).start()

    def project_some(count, slot_of):
        def body(i, carry):
            project(slot_of(i))
            return carry
        lax.fori_loop(0, count, body, 0)

    for k in range(7):
        tr[k].wait_recv()
        tl[k].wait_recv()
        if k < 4:
            for c in oz[k + 1]:
                c.wait_recv()
            if k < 3:
                oz[k + 2] = hop(k + 2)
        if k < 5:
            tr[k + 2] = tright(k + 2)
            tl[k + 2] = tleft(k + 2)
        if k == 0:
            ax = one("a", AX)
            wya.forward()
            wxb.forward()
        if k == 1:
            bx = one("b", BX)
            ax.finish()
            ay = two("a", AY, 0)
            normalize(1)
            normalize(7)
            wya.finish()
            wxb.finish()
        if k == 2:
            bx.finish()
            by = two("b", BY, 8)
            for c in wd:
                c.wait_recv()
            project_some(3, lambda i: lax.rem(i + 7, 8))
        if k == 3:
            cx = one("c", CX)
            ay.forward()
            normalize(2)
            normalize(6)
            project_some(2, lambda i: 2 + 4 * i)
        if k == 4:
            by.forward()
            cx.finish()
            cy = two("c", CY, 16)
        if k == 5:
            ay.finish()
            normalize(3)
            normalize(5)
            project_some(2, lambda i: 3 + 2 * i)
        if k == 6:
            normalize(4)
            project_some(1, lambda i: i + 4)
            cy.forward()
            by.finish()

    for slot in range(8):
        rc(kv.at[slot], kv.at[8 + slot], KX + slot, xpeer[2]).wait_recv()

    unit = 1.0 / math.sqrt(128)

    def attend(i, carry):
        a, b = 4 + i, 3 - i
        for h in range(2):
            hc = slice(h * 128, (h + 1) * 128)
            q = jnp.concatenate([qs[a, :, hc], qs[b, :, hc]], axis=0)
            keys = kv[:, :, h * 256:h * 256 + 128].reshape(2048, 128)
            vals = kv[:, :, h * 256 + 128:h * 256 + 256].reshape(2048, 128)
            sc = lax.dot_general(q, keys, (((1,), (1,)), ((), ())), preferred_element_type=F32)
            top = jnp.max(sc, axis=1, keepdims=True)
            e = jnp.exp((sc - top) * unit)
            total = jnp.sum(e, axis=1, keepdims=True)
            o = jnp.dot(e.astype(BF), vals, preferred_element_type=F32) / total
            o = o.astype(BF)
            at[a, :, hc] = o[:128]
            at[b, :, hc] = o[128:]
        rc(at.at[a], mx.at[8 - a], AZ + a, dev(lax.rem(z + 8 - a, 8), x, y, core)).start()

        @pl.when(i < 3)
        def _():
            rc(at.at[b], mx.at[8 - b], AZ + b, dev(lax.rem(z + 8 - b, 8), x, y, core)).start()

        return carry

    lax.fori_loop(0, 4, attend, 0)
    mx[0] = at[0]

    az = {d: rc(at.at[d], mx.at[8 - d], AZ + d, dev(lax.rem(z + 8 - d, 8), x, y, core)) for d in range(1, 8)}

    def out_copy(q):
        return pltpu.make_async_copy(
            res.at[q], out_hbm.at[:, pl.ds(q * 768, 768)], ls.at[q])

    cy.finish()
    for c in od:
        c.wait_recv()
    for n, pair in enumerate(((4, 3), (5, 2), (6, 1), (7, 0))):
        for d in pair:
            if d > 0:
                az[d].wait_recv()
        ta, tb = ((8 - d) % 8 for d in pair)
        pa, pb = PLACE[ta], PLACE[tb]

        def out_part(q, carry):
            m = jnp.concatenate([mx[ta], mx[tb]], axis=1)
            w = jnp.concatenate([wo[q, pa].reshape(256, 768), wo[q, pb].reshape(256, 768)], axis=0)
            part_sum = jnp.dot(m, w, preferred_element_type=F32)
            if n > 0:
                part_sum += acc[q]
            if n < 3:
                acc[q] = part_sum
            else:
                res[q] = (part_sum * mod[8 + q][0:1]).astype(BF)
            return carry

        if n < 3:
            lax.fori_loop(0, 4, out_part, 0)
        else:
            for q in range(4):
                out_part(q, 0)
                out_copy(q).start()

    for q in range(4):
        out_copy(q).wait()
    for c in sent:
        c.wait_send()
    for slot in range(8):
        rc(kv.at[slot], kv.at[8 + slot], KX + slot, xpeer[2]).wait_send()
    for c in az.values():
        c.wait_send()


def on_device(latents, timestep, w_mod, w_qkv, w_out):
    half_freq = w_mod.shape[0] // 2
    freqs = jnp.exp(-math.log(10000.0) * jnp.arange(half_freq, dtype=F32) / half_freq)
    angles = timestep.astype(F32)[:, None] * freqs[None, :]
    embed = jnp.concatenate([jnp.cos(angles), jnp.sin(angles)], axis=1).astype(BF)
    embed = jnp.broadcast_to(embed, (16, 2 * half_freq))
    anyspace = pl.BlockSpec(memory_space=pl.ANY)
    out = pl.pallas_call(
        kernel,
        out_shape=jax.ShapeDtypeStruct((128, 3072), BF),
        in_specs=[pl.BlockSpec(memory_space=pltpu.VMEM)] + [anyspace] * 4,
        out_specs=anyspace,
        scratch_shapes=[
            pltpu.VMEM((256, 9216), BF),
            pltpu.VMEM((12, 16, 768), F32),
            pltpu.VMEM((8, 128, 3072), BF),
            pltpu.VMEM((8, 128, 3072), BF),
            pltpu.VMEM((2, 4, 2, 192, 768), BF),
            pltpu.VMEM((4, 8, 2, 2, 4, 16, 768), BF),
            pltpu.VMEM((8, 3072), BF),
            pltpu.VMEM((8, 3072), BF),
            pltpu.VMEM((8, 128, 256), BF),
            pltpu.VMEM((16, 128, 512), BF),
            pltpu.VMEM((8, 128, 256), BF),
            pltpu.VMEM((8, 128, 256), BF),
            pltpu.VMEM((4, 128, 768), F32),
            pltpu.VMEM((4, 128, 768), BF),
            pltpu.SemaphoreType.DMA((COUNT,)),
            pltpu.SemaphoreType.DMA((COUNT,)),
            pltpu.SemaphoreType.DMA((5,)),
        ],
        compiler_params=pltpu.CompilerParams(
            collective_id=0, has_side_effects=True, vmem_limit_bytes=60 * 1024 * 1024,
        ),
        name="sublayer",
    )(embed, latents[0], w_mod, w_qkv[0], w_out[0])
    return out[None]


def solution(mesh):
    placed = (P("grp", "sp", None), P("grp"), P(), P("sp", "grp", None), P("sp", "grp", None))
    return jax.shard_map(
        on_device, mesh=mesh, in_specs=placed, out_specs=P("grp", "sp", None), check_vma=False
    )
```

```python
import functools
import math

import jax
import jax.numpy as jnp
from jax import lax
from jax.experimental import pallas as pl
from jax.experimental.pallas import tpu as pltpu
from jax.sharding import PartitionSpec as P

MESH = pl.DeviceIdType.MESH
BF = jnp.bfloat16
F32 = jnp.float32

TR, TL, WXA, WYA, WYB, WXB, WD, OP, OZR, OZL = 0, 8, 16, 20, 26, 30, 36, 52, 53, 58
AX, AY, BX, BY, CX, CY, OD, KX, AZ, COUNT = 63, 67, 73, 77, 83, 87, 93, 117, 127, 135

PLACE = (0, 1, 3, 5, 7, 6, 4, 2)


class Direct:
    def __init__(self, send, ref, base, peers):
        self.copies = [send(ref, ref, base + o, peers[o]) for o in (2, 1, 3)]

    def finish(self):
        for c in self.copies:
            c.wait_recv()


class Ring:
    def __init__(self, send, region, me, base, plus, minus, landed=None):
        self.send, self.region, self.base = send, region, base
        self.me, self.plus, self.minus = me, plus, minus
        self.landed = landed
        self.copies = {}
        for k, half, to in ((0, 0, plus), (2, 1, minus), (1, 1, plus), (3, 0, minus)):
            self.go(k, 0, half, to)
        if landed:
            landed(me, 0, 0)
            landed(me, 1, 1)

    def go(self, k, shift, half, to):
        ref = self.region(lax.rem(self.me + shift, 4), half)
        self.copies[k] = self.send(ref, ref, self.base + k, to)

    def arrive(self, k, shift, half, n):
        self.copies[k].wait_recv()
        if self.landed:
            self.landed(lax.rem(self.me + shift, 4), half, n)

    def forward(self):
        self.copies[0].wait_recv()
        self.go(4, 3, 0, self.plus)
        self.copies[2].wait_recv()
        self.go(5, 1, 1, self.minus)
        if self.landed:
            self.landed(lax.rem(self.me + 3, 4), 0, 2)
            self.landed(lax.rem(self.me + 1, 4), 1, 3)

    def near(self):
        self.arrive(1, 3, 1, 4)
        self.arrive(3, 1, 0, 5)

    def far(self):
        self.arrive(4, 2, 0, 6)
        self.arrive(5, 2, 1, 7)

    def finish(self):
        self.near()
        self.far()


def kernel(embed, lat_hbm, wm_hbm, wqkv_hbm, wout_hbm, out_hbm,
           wm, mod, tok, nrm, wq, wo, pw_own, pw_par, qs, kv, at, mx, acc, res,
           ss, rs, ls):
    s = lax.axis_index("sp")
    g = lax.axis_index("grp")
    z, xh = lax.div(s, 2), lax.rem(s, 2)
    xl, y, core = lax.div(g, 8), lax.rem(lax.div(g, 2), 4), lax.rem(g, 2)
    x = xh * 2 + xl

    def dev(zz, xx, yy, cc):
        grp = (lax.rem(xx, 2) * 4 + yy) * 2 + cc
        return (grp, zz * 2 + lax.div(xx, 2))

    zpeer = {o: dev(lax.rem(z + o, 8), x, y, core) for o in range(1, 8)}
    xpeer = {o: dev(z, lax.rem(x + o, 4), y, core) for o in range(1, 4)}
    ypeer = {o: dev(z, x, lax.rem(y + o, 4), core) for o in range(1, 4)}
    partner = dev(z, x, y, 1 - core)
    right, left = zpeer[1], zpeer[7]

    def rc(src, dst, i, to):
        return pltpu.make_async_remote_copy(
            src_ref=src, dst_ref=dst, send_sem=ss.at[i], recv_sem=rs.at[i],
            device_id=to, device_id_type=MESH,
        )

    sent = []

    def send(*args):
        copy = rc(*args)
        copy.start()
        sent.append(copy)
        return copy

    cols = pl.ds(pl.multiple_of(xh * 384, 128), 384)
    own_w = wq.at[xl, y, core, :, cols]

    c_w = pltpu.make_async_copy(wqkv_hbm, own_w, ls.at[0])
    c_o = pltpu.make_async_copy(wout_hbm, pw_own, ls.at[1])
    c_x = pltpu.make_async_copy(lat_hbm, tok.at[0], ls.at[2])
    c_m = pltpu.make_async_copy(wm_hbm, wm, ls.at[3])
    for c in (c_x, c_w, c_o, c_m):
        c.start()

    barrier = pltpu.get_barrier_semaphore()
    for p in (*zpeer.values(), *xpeer.values(), *ypeer.values(), partner):
        pl.semaphore_signal(barrier, inc=1, device_id=p, device_id_type=MESH)
    c_x.wait()
    c_w.wait()
    c_o.wait()
    pl.semaphore_wait(barrier, 14)

    part = (pl.ds(0, 64), pl.ds(64, 64))

    def right_copy(k):
        d = k // 2
        rows = part[k % 2] if d < 3 else pl.ds(32 * (7 - k), 32)
        return rc(tok.at[d, rows], tok.at[d + 1, rows], TR + k, right)

    def left_copy(k):
        d = k // 2
        rows = part[1 - k % 2] if d < 3 else pl.ds(64 + 32 * (k - 6), 32)
        return rc(tok.at[(8 - d) % 8, rows], tok.at[7 - d, rows], TL + k, left)

    tr = {k: right_copy(k) for k in range(8)}
    tl = {k: left_copy(k) for k in range(8)}
    sent.extend([*tr.values(), *tl.values()])

    def pass_on(k):
        tr[k].start()
        tl[k].start()

    pass_on(0)


    op = send(pw_own, pw_par, OP, partner)
    top, low = pl.ds(0, 96), pl.ds(96, 96)
    wxa = Direct(send, wq.at[xl, y, core, top, cols], WXA, xpeer)
    wyb = Direct(send, wq.at[xl, y, core, low, cols], WYB, ypeer)

    op.wait_recv()
    first = core == 0
    for j in range(2):
        def half(ref):
            a = ref[:, j * 768:(j + 1) * 768].astype(F32)
            b = ref[:, 1536 + j * 768:1536 + (j + 1) * 768].astype(F32)
            return jnp.where(first, a, b)
        a, b = half(pw_own), half(pw_par)
        rows = jnp.concatenate([jnp.where(first, a, b), jnp.where(first, b, a)], axis=0)
        wo[core * 2 + j, 0, xh, xl, y] = rows.astype(BF)

    def slab(slot, far):
        quarter = pl.ds(core * 2, 2) if far is None else core * 2 + far
        return wo.at[quarter, PLACE[slot], xh, xl, y]

    def hop(h):
        r, l = (0, 1) if h == 4 else (None, None)
        return (send(slab(h - 1, r), slab(h, r), OZR + h, right),
                send(slab((9 - h) % 8, l), slab(8 - h, l), OZL + h, left))

    oz = {1: hop(1)}

    pass_on(1)


    c_m.wait()
    wave = jnp.broadcast_to(embed[...].astype(F32), (16, 256)).astype(BF)
    for j in range(12):
        mod[j] = jnp.dot(wave, wm[:, j * 768:(j + 1) * 768], preferred_element_type=F32)

    def normalize(slot, lo=0, hi=8):
        def rows(i, carry):
            r = pl.ds(pl.multiple_of(i * 16, 16), 16)
            v = tok[slot, r, :].astype(F32)
            center = jnp.sum(v, axis=-1, keepdims=True) * (1.0 / 3072)
            v = v - center
            spread = jnp.sum(v * v, axis=-1, keepdims=True) * (1.0 / 3072)
            v = v * lax.rsqrt(spread + 1e-06)
            for j in range(4):
                c = slice(j * 768, (j + 1) * 768)
                nrm[slot, r, c] = (v[:, c] * (1.0 + mod[4 + j]) + mod[j]).astype(BF)
            return carry
        lax.fori_loop(lo, hi, rows, 0)

    wd = []

    def wya_region(i, h):
        return wq.at[h, i, core, top]

    def wxb_region(i, h):
        c = pl.ds(pl.multiple_of(lax.div(i, 2) * 384, 128), 384)
        return wq.at[lax.rem(i, 2), pl.ds(h * 2, 2), core, low, c]

    def w_landed(region, base):
        def landed(i, h, n):
            ref = region(i, h)
            wd.append(send(ref, ref, base + n, partner))
        return landed

    wxa.finish()
    wya = Ring(send, wya_region, y, WYA, ypeer[1], ypeer[3], w_landed(wya_region, WD))
    wyb.finish()
    wxb = Ring(send, wxb_region, x, WXB, xpeer[1], xpeer[3], w_landed(wxb_region, WD + 8))
    normalize(0)

    groups = {"a": pl.ds(0, 3), "b": pl.ds(3, 2), "c": pl.ds(5, 3)}
    od = []

    def one(name, base):
        return Direct(send, wo.at[pl.ds(core * 2, 2), groups[name], xh, xl, y], base, xpeer)

    def two(name, base, first_od):
        def region(i, h):
            return wo.at[core * 2 + h, groups[name], :, :, i]

        def landed(i, h, n):
            ref = region(i, h)
            od.append(send(ref, ref, OD + first_od + n, partner))

        return Ring(send, region, y, base, ypeer[1], ypeer[3], landed)

    def project(slot):
        acc = jnp.zeros((128, 768), F32)
        for a in range(2):
            w = wq[a].reshape(1536, 768)
            acc += jnp.dot(nrm[slot, :, a * 1536:(a + 1) * 1536], w, preferred_element_type=F32)
        acc = acc.astype(BF)
        qs[slot, :, 0:128] = acc[:, 0:128]
        qs[slot, :, 128:256] = acc[:, 384:512]
        kv[slot, :, 0:256] = acc[:, 128:384]
        kv[slot, :, 256:512] = acc[:, 512:768]
        rc(kv.at[slot], kv.at[8 + slot], KX + slot, xpeer[2]).start()

    kv_last = {
        r: rc(kv.at[4, pl.ds(r, n)], kv.at[12, pl.ds(r, n)], KX + i, xpeer[2])
        for i, r, n in ((4, 32, 64), (8, 0, 32), (9, 96, 32))
    }

    def project_last(starts):
        acc = jnp.zeros((64, 768), F32)
        size = 64 // len(starts)
        for a in range(2):
            w = wq[a].reshape(1536, 768)
            cut = slice(a * 1536, (a + 1) * 1536)
            rows = jnp.concatenate([nrm[4, r:r + size, cut] for r in starts], axis=0)
            acc += jnp.dot(rows, w, preferred_element_type=F32)
        acc = acc.astype(BF)
        for n, r in enumerate(starts):
            one = acc[n * size:(n + 1) * size]
            qs[4, r:r + size, 0:128] = one[:, 0:128]
            qs[4, r:r + size, 128:256] = one[:, 384:512]
            kv[4, r:r + size, 0:256] = one[:, 128:384]
            kv[4, r:r + size, 256:512] = one[:, 512:768]
            kv_last[r].start()

    def project_some(count, slot_of):
        def body(i, carry):
            project(slot_of(i))
            return carry
        lax.fori_loop(0, count, body, 0)

    for k in range(7):
        tr[k].wait_recv()
        tl[k].wait_recv()
        if k < 4:
            for c in oz[k + 1]:
                c.wait_recv()
            if k < 3:
                oz[k + 2] = hop(k + 2)
        if k < 5:
            pass_on(k + 2)
        if k == 4:
            pass_on(7)
        if k == 0:
            ax = one("a", AX)
            wya.forward()
            wxb.forward()
        if k == 1:
            bx = one("b", BX)
            ax.finish()
            ay = two("a", AY, 0)
            normalize(1)
            normalize(7)
            wya.finish()
            wxb.finish()
        if k == 2:
            bx.finish()
            by = two("b", BY, 8)
            for c in wd:
                c.wait_recv()
            project_some(3, lambda i: lax.rem(i + 7, 8))
        if k == 3:
            cx = one("c", CX)
            ay.forward()
            normalize(2)
            normalize(6)
            project_some(2, lambda i: 2 + 4 * i)
        if k == 4:
            by.forward()
            cx.finish()
            cy = two("c", CY, 16)
        if k == 5:
            ay.finish()
            normalize(3)
            normalize(5)
            project_some(2, lambda i: 3 + 2 * i)
            cy.forward()
        if k == 6:
            normalize(4, 2, 6)
            project_last((32,))
            tr[7].wait_recv()
            tl[7].wait_recv()
            normalize(4, 0, 2)
            normalize(4, 6, 8)
            project_last((0, 96))
            by.finish()

    kv_all = [rc(kv.at[d], kv.at[8 + d], KX + d, xpeer[2]) for d in range(8) if d != 4]
    kv_all.extend(kv_last.values())
    for c in kv_all:
        c.wait_recv()

    unit = math.log2(math.e) / math.sqrt(128)

    def attend(i, carry):
        a, b = 4 + i, lax.rem(4 - i, 4)
        for h in range(2):
            hc = slice(h * 128, (h + 1) * 128)
            q = jnp.concatenate([qs[a, :, hc], qs[b, :, hc]], axis=0)
            keys = kv[:, :, h * 256:h * 256 + 128].reshape(2048, 128)
            vals = kv[:, :, h * 256 + 128:h * 256 + 256].reshape(2048, 128)
            sc = lax.dot_general(q, keys, (((1,), (1,)), ((), ())), preferred_element_type=F32)
            top = jnp.max(sc, axis=1, keepdims=True)
            e = jnp.exp2((sc - top) * unit)
            total = jnp.sum(e, axis=1, keepdims=True)
            o = jnp.dot(e.astype(BF), vals, preferred_element_type=F32) / total
            o = o.astype(BF)
            at[a, :, hc] = o[:128]
            at[b, :, hc] = o[128:]
        rc(at.at[a], mx.at[8 - a], AZ + a, dev(lax.rem(z + 8 - a, 8), x, y, core)).start()

        @pl.when(i > 0)
        def _():
            rc(at.at[b], mx.at[8 - b], AZ + b, dev(lax.rem(z + 8 - b, 8), x, y, core)).start()

        return carry

    lax.fori_loop(0, 4, attend, 0)
    mx[0] = at[0]

    az = {d: rc(at.at[d], mx.at[8 - d], AZ + d, dev(lax.rem(z + 8 - d, 8), x, y, core)) for d in range(1, 8)}

    def out_copy(q):
        return pltpu.make_async_copy(
            res.at[q], out_hbm.at[:, pl.ds(q * 768, 768)], ls.at[q])

    cy.finish()
    for c in od:
        c.wait_recv()
    for n, pair in enumerate(((4, 0), (5, 3), (6, 2), (7, 1))):
        for d in pair:
            if d > 0:
                az[d].wait_recv()
        ta, tb = ((8 - d) % 8 for d in pair)
        pa, pb = PLACE[ta], PLACE[tb]

        def out_part(q, carry):
            m = jnp.concatenate([mx[ta], mx[tb]], axis=1)
            w = jnp.concatenate([wo[q, pa].reshape(256, 768), wo[q, pb].reshape(256, 768)], axis=0)
            part_sum = jnp.dot(m, w, preferred_element_type=F32)
            if n > 0:
                part_sum += acc[q]
            if n < 3:
                acc[q] = part_sum
            else:
                res[q] = (part_sum * mod[8 + q][0:1]).astype(BF)
            return carry

        if n < 3:
            lax.fori_loop(0, 4, out_part, 0)
        else:
            for q in range(4):
                out_part(q, 0)
                out_copy(q).start()

    for q in range(4):
        out_copy(q).wait()
    for c in sent:
        c.wait_send()
    for c in kv_all:
        c.wait_send()
    for c in az.values():
        c.wait_send()


def on_device(latents, timestep, w_mod, w_qkv, w_out):
    half_freq = w_mod.shape[0] // 2
    freqs = jnp.exp(-math.log(10000.0) * jnp.arange(half_freq, dtype=F32) / half_freq)
    angles = timestep.astype(F32)[:, None] * freqs[None, :]
    embed = jnp.concatenate([jnp.cos(angles), jnp.sin(angles)], axis=1).astype(BF)
    anyspace = pl.BlockSpec(memory_space=pl.ANY)
    out = pl.pallas_call(
        kernel,
        out_shape=jax.ShapeDtypeStruct((128, 3072), BF),
        in_specs=[pl.BlockSpec(memory_space=pltpu.VMEM)] + [anyspace] * 4,
        out_specs=anyspace,
        scratch_shapes=[
            pltpu.VMEM((256, 9216), BF),
            pltpu.VMEM((12, 16, 768), F32),
            pltpu.VMEM((8, 128, 3072), BF),
            pltpu.VMEM((8, 128, 3072), BF),
            pltpu.VMEM((2, 4, 2, 192, 768), BF),
            pltpu.VMEM((4, 8, 2, 2, 4, 16, 768), BF),
            pltpu.VMEM((8, 3072), BF),
            pltpu.VMEM((8, 3072), BF),
            pltpu.VMEM((8, 128, 256), BF),
            pltpu.VMEM((16, 128, 512), BF),
            pltpu.VMEM((8, 128, 256), BF),
            pltpu.VMEM((8, 128, 256), BF),
            pltpu.VMEM((4, 128, 768), F32),
            pltpu.VMEM((4, 128, 768), BF),
            pltpu.SemaphoreType.DMA((COUNT,)),
            pltpu.SemaphoreType.DMA((COUNT,)),
            pltpu.SemaphoreType.DMA((5,)),
        ],
        compiler_params=pltpu.CompilerParams(
            collective_id=0, has_side_effects=True, vmem_limit_bytes=60 * 1024 * 1024,
        ),
        name="sublayer",
    )(embed, latents[0], w_mod, w_qkv[0], w_out[0])
    return out[None]


def solution(mesh):
    placed = (P("grp", "sp", None), P("grp"), P(), P("sp", "grp", None), P("sp", "grp", None))
    return jax.shard_map(
        on_device, mesh=mesh, in_specs=placed, out_specs=P("grp", "sp", None), check_vma=False
    )
```

```python
import functools
import math

import jax
import jax.numpy as jnp
from jax import lax
from jax.experimental import pallas as pl
from jax.experimental.pallas import tpu as pltpu
from jax.sharding import PartitionSpec as P

MESH = pl.DeviceIdType.MESH
BF = jnp.bfloat16
F32 = jnp.float32

TR, TL, WXA, WYA, WYB, WXB, WD, OP, OZR, OZL = 0, 8, 16, 20, 26, 30, 36, 52, 53, 58
AX, AY, BX, BY, CX, CY, OD, KX, AZ, COUNT = 63, 67, 73, 77, 83, 87, 93, 117, 127, 135

PLACE = (0, 1, 3, 5, 7, 6, 4, 2)


class Direct:
    def __init__(self, send, ref, base, peers):
        self.copies = [send(ref, ref, base + o, peers[o]) for o in (2, 1, 3)]

    def finish(self):
        for c in self.copies:
            c.wait_recv()


class Ring:
    def __init__(self, send, region, me, base, plus, minus, landed=None):
        self.send, self.region, self.base = send, region, base
        self.me, self.plus, self.minus = me, plus, minus
        self.landed = landed
        self.copies = {}
        for k, half, to in ((0, 0, plus), (2, 1, minus), (1, 1, plus), (3, 0, minus)):
            self.go(k, 0, half, to)
        if landed:
            landed(me, 0, 0)
            landed(me, 1, 1)

    def go(self, k, shift, half, to):
        ref = self.region(lax.rem(self.me + shift, 4), half)
        self.copies[k] = self.send(ref, ref, self.base + k, to)

    def arrive(self, k, shift, half, n):
        self.copies[k].wait_recv()
        if self.landed:
            self.landed(lax.rem(self.me + shift, 4), half, n)

    def forward(self):
        self.copies[0].wait_recv()
        self.go(4, 3, 0, self.plus)
        self.copies[2].wait_recv()
        self.go(5, 1, 1, self.minus)
        if self.landed:
            self.landed(lax.rem(self.me + 3, 4), 0, 2)
            self.landed(lax.rem(self.me + 1, 4), 1, 3)

    def near(self):
        self.arrive(1, 3, 1, 4)
        self.arrive(3, 1, 0, 5)

    def far(self):
        self.arrive(4, 2, 0, 6)
        self.arrive(5, 2, 1, 7)

    def finish(self):
        self.near()
        self.far()


def kernel(embed, lat_hbm, wm_hbm, wqkv_hbm, wout_hbm, out_hbm,
           wm, mod, tok, nrm, wq, wo, pw_own, pw_par, qs, kv, at, mx, acc, res,
           ss, rs, ls):
    s = lax.axis_index("sp")
    g = lax.axis_index("grp")
    z, xh = lax.div(s, 2), lax.rem(s, 2)
    xl, y, core = lax.div(g, 8), lax.rem(lax.div(g, 2), 4), lax.rem(g, 2)
    x = xh * 2 + xl

    def dev(zz, xx, yy, cc):
        grp = (lax.rem(xx, 2) * 4 + yy) * 2 + cc
        return (grp, zz * 2 + lax.div(xx, 2))

    zpeer = {o: dev(lax.rem(z + o, 8), x, y, core) for o in range(1, 8)}
    xpeer = {o: dev(z, lax.rem(x + o, 4), y, core) for o in range(1, 4)}
    ypeer = {o: dev(z, x, lax.rem(y + o, 4), core) for o in range(1, 4)}
    partner = dev(z, x, y, 1 - core)
    right, left = zpeer[1], zpeer[7]

    def rc(src, dst, i, to):
        return pltpu.make_async_remote_copy(
            src_ref=src, dst_ref=dst, send_sem=ss.at[i], recv_sem=rs.at[i],
            device_id=to, device_id_type=MESH,
        )

    sent = []

    def send(*args):
        copy = rc(*args)
        copy.start()
        sent.append(copy)
        return copy

    cols = pl.ds(pl.multiple_of(xh * 384, 128), 384)
    own_w = wq.at[xl, y, core, :, cols]

    c_w = pltpu.make_async_copy(wqkv_hbm, own_w, ls.at[0])
    c_o = pltpu.make_async_copy(wout_hbm, pw_own, ls.at[1])
    c_x = pltpu.make_async_copy(lat_hbm, tok.at[0], ls.at[2])
    c_m = pltpu.make_async_copy(wm_hbm, wm, ls.at[3])
    for c in (c_x, c_w, c_o, c_m):
        c.start()

    barrier = pltpu.get_barrier_semaphore()
    for p in (*zpeer.values(), *xpeer.values(), *ypeer.values(), partner):
        pl.semaphore_signal(barrier, inc=1, device_id=p, device_id_type=MESH)
    c_x.wait()
    c_w.wait()
    c_o.wait()
    pl.semaphore_wait(barrier, 14)

    part = (pl.ds(0, 64), pl.ds(64, 64))

    def right_copy(k):
        d = k // 2
        rows = part[k % 2] if d < 3 else pl.ds(32 * (7 - k), 32)
        return rc(tok.at[d, rows], tok.at[d + 1, rows], TR + k, right)

    def left_copy(k):
        d = k // 2
        rows = part[1 - k % 2] if d < 3 else pl.ds(64 + 32 * (k - 6), 32)
        return rc(tok.at[(8 - d) % 8, rows], tok.at[7 - d, rows], TL + k, left)

    tr = {k: right_copy(k) for k in range(8)}
    tl = {k: left_copy(k) for k in range(8)}
    sent.extend([*tr.values(), *tl.values()])

    def pass_on(k):
        tr[k].start()
        tl[k].start()

    pass_on(0)


    op = send(pw_own, pw_par, OP, partner)
    top, low = pl.ds(0, 96), pl.ds(96, 96)
    wxa = Direct(send, wq.at[xl, y, core, top, cols], WXA, xpeer)
    wyb = Direct(send, wq.at[xl, y, core, low, cols], WYB, ypeer)

    op.wait_recv()
    first = core == 0
    for j in range(2):
        def half(ref):
            a = ref[:, j * 768:(j + 1) * 768].astype(F32)
            b = ref[:, 1536 + j * 768:1536 + (j + 1) * 768].astype(F32)
            return jnp.where(first, a, b)
        a, b = half(pw_own), half(pw_par)
        rows = jnp.concatenate([jnp.where(first, a, b), jnp.where(first, b, a)], axis=0)
        wo[core * 2 + j, 0, xh, xl, y] = rows.astype(BF)

    def slab(slot, far):
        quarter = pl.ds(core * 2, 2) if far is None else core * 2 + far
        return wo.at[quarter, PLACE[slot], xh, xl, y]

    def hop(h):
        r, l = (0, 1) if h == 4 else (None, None)
        return (send(slab(h - 1, r), slab(h, r), OZR + h, right),
                send(slab((9 - h) % 8, l), slab(8 - h, l), OZL + h, left))

    oz = {1: hop(1)}

    pass_on(1)


    c_m.wait()
    wave = jnp.broadcast_to(embed[...].astype(F32), (16, 256)).astype(BF)
    for j in range(12):
        mod[j] = jnp.dot(wave, wm[:, j * 768:(j + 1) * 768], preferred_element_type=F32)

    def normalize(slot, lo=0, hi=8):
        def rows(i, carry):
            r = pl.ds(pl.multiple_of(i * 16, 16), 16)
            v = tok[slot, r, :].astype(F32)
            center = jnp.sum(v, axis=-1, keepdims=True) * (1.0 / 3072)
            v = v - center
            spread = jnp.sum(v * v, axis=-1, keepdims=True) * (1.0 / 3072)
            v = v * lax.rsqrt(spread + 1e-06)
            for j in range(4):
                c = slice(j * 768, (j + 1) * 768)
                nrm[slot, r, c] = (v[:, c] * (1.0 + mod[4 + j]) + mod[j]).astype(BF)
            return carry
        lax.fori_loop(lo, hi, rows, 0)

    wd = []

    def wya_region(i, h):
        return wq.at[h, i, core, top]

    def wxb_region(i, h):
        c = pl.ds(pl.multiple_of(lax.div(i, 2) * 384, 128), 384)
        return wq.at[lax.rem(i, 2), pl.ds(h * 2, 2), core, low, c]

    def w_landed(region, base):
        def landed(i, h, n):
            ref = region(i, h)
            wd.append(send(ref, ref, base + n, partner))
        return landed

    wxa.finish()
    wya = Ring(send, wya_region, y, WYA, ypeer[1], ypeer[3], w_landed(wya_region, WD))
    wyb.finish()
    wxb = Ring(send, wxb_region, x, WXB, xpeer[1], xpeer[3], w_landed(wxb_region, WD + 8))
    normalize(0)

    groups = {"a": pl.ds(0, 3), "b": pl.ds(3, 2), "c": pl.ds(5, 3)}
    od = []

    def one(name, base):
        return Direct(send, wo.at[pl.ds(core * 2, 2), groups[name], xh, xl, y], base, xpeer)

    def two(name, base, first_od):
        def region(i, h):
            return wo.at[core * 2 + h, groups[name], :, :, i]

        def landed(i, h, n):
            ref = region(i, h)
            od.append(send(ref, ref, OD + first_od + n, partner))

        return Ring(send, region, y, base, ypeer[1], ypeer[3], landed)

    def project(slot):
        acc = jnp.zeros((128, 768), F32)
        for a in range(2):
            w = wq[a].reshape(1536, 768)
            acc += jnp.dot(nrm[slot, :, a * 1536:(a + 1) * 1536], w, preferred_element_type=F32)
        acc = acc.astype(BF)
        qs[slot, :, 0:128] = acc[:, 0:128]
        qs[slot, :, 128:256] = acc[:, 384:512]
        kv[slot, :, 0:256] = acc[:, 128:384]
        kv[slot, :, 256:512] = acc[:, 512:768]
        rc(kv.at[slot], kv.at[8 + slot], KX + slot, xpeer[2]).start()

    kv_last = {
        r: rc(kv.at[4, pl.ds(r, n)], kv.at[12, pl.ds(r, n)], KX + i, xpeer[2])
        for i, r, n in ((4, 32, 64), (8, 0, 32), (9, 96, 32))
    }

    def project_last(starts):
        size = 64 // len(starts)

        def columns(*spans):
            acc = jnp.zeros((64, 128 * len(spans)), F32)
            for a in range(2):
                cut = slice(a * 1536, (a + 1) * 1536)
                w = jnp.concatenate(
                    [wq[a, :, :, :, c:c + 128].reshape(1536, 128) for c in spans], axis=1)
                rows = jnp.concatenate([nrm[4, r:r + size, cut] for r in starts], axis=0)
                acc += jnp.dot(rows, w, preferred_element_type=F32)
            return acc.astype(BF)

        pairs = columns(128, 256, 512, 640)
        for n, r in enumerate(starts):
            kv[4, r:r + size, :] = pairs[n * size:(n + 1) * size]
            kv_last[r].start()
        asks = columns(0, 384)
        for n, r in enumerate(starts):
            qs[4, r:r + size, :] = asks[n * size:(n + 1) * size]

    def project_some(count, slot_of):
        def body(i, carry):
            project(slot_of(i))
            return carry
        lax.fori_loop(0, count, body, 0)

    for k in range(7):
        tr[k].wait_recv()
        tl[k].wait_recv()
        if k < 4:
            for c in oz[k + 1]:
                c.wait_recv()
            if k < 3:
                oz[k + 2] = hop(k + 2)
        if k < 5:
            pass_on(k + 2)
        if k == 4:
            pass_on(7)
        if k == 0:
            ax = one("a", AX)
            wya.forward()
            wxb.forward()
        if k == 1:
            bx = one("b", BX)
            ax.finish()
            ay = two("a", AY, 0)
            normalize(1)
            normalize(7)
            wya.finish()
            wxb.finish()
        if k == 2:
            bx.finish()
            by = two("b", BY, 8)
            for c in wd:
                c.wait_recv()
            project_some(3, lambda i: lax.rem(i + 7, 8))
        if k == 3:
            cx = one("c", CX)
            ay.forward()
            normalize(2)
            normalize(6)
            project_some(2, lambda i: 2 + 4 * i)
        if k == 4:
            by.forward()
            cx.finish()
            cy = two("c", CY, 16)
        if k == 5:
            ay.finish()
            normalize(3)
            normalize(5)
            project_some(2, lambda i: 3 + 2 * i)
            cy.forward()
        if k == 6:
            normalize(4, 2, 6)
            project_last((32,))
            tr[7].wait_recv()
            tl[7].wait_recv()
            normalize(4, 0, 2)
            normalize(4, 6, 8)
            project_last((0, 96))
            by.finish()

    kv_all = [rc(kv.at[d], kv.at[8 + d], KX + d, xpeer[2]) for d in range(8) if d != 4]
    kv_all.extend(kv_last.values())
    for c in kv_all:
        c.wait_recv()

    unit = math.log2(math.e) / math.sqrt(128)

    def attend(i, carry):
        a, b = 4 + i, lax.rem(4 - i, 4)
        for h in range(2):
            hc = slice(h * 128, (h + 1) * 128)
            q = jnp.concatenate([qs[a, :, hc], qs[b, :, hc]], axis=0)
            keys = kv[:, :, h * 256:h * 256 + 128].reshape(2048, 128)
            vals = kv[:, :, h * 256 + 128:h * 256 + 256].reshape(2048, 128)
            sc = lax.dot_general(q, keys, (((1,), (1,)), ((), ())), preferred_element_type=F32)
            top = jnp.max(sc, axis=1, keepdims=True)
            e = jnp.exp2((sc - top) * unit)
            total = jnp.sum(e, axis=1, keepdims=True)
            o = jnp.dot(e.astype(BF), vals, preferred_element_type=F32) / total
            o = o.astype(BF)
            at[a, :, hc] = o[:128]
            at[b, :, hc] = o[128:]
        rc(at.at[a], mx.at[8 - a], AZ + a, dev(lax.rem(z + 8 - a, 8), x, y, core)).start()

        @pl.when(i > 0)
        def _():
            rc(at.at[b], mx.at[8 - b], AZ + b, dev(lax.rem(z + 8 - b, 8), x, y, core)).start()

        return carry

    lax.fori_loop(0, 4, attend, 0)
    mx[0] = at[0]

    az = {d: rc(at.at[d], mx.at[8 - d], AZ + d, dev(lax.rem(z + 8 - d, 8), x, y, core)) for d in range(1, 8)}

    def out_copy(q):
        return pltpu.make_async_copy(
            res.at[q], out_hbm.at[:, pl.ds(q * 768, 768)], ls.at[q])

    cy.finish()
    for c in od:
        c.wait_recv()
    for n, pair in enumerate(((4, 0), (5, 3), (6, 2), (7, 1))):
        for d in pair:
            if d > 0:
                az[d].wait_recv()
        ta, tb = ((8 - d) % 8 for d in pair)
        pa, pb = PLACE[ta], PLACE[tb]

        def out_part(q, carry):
            m = jnp.concatenate([mx[ta], mx[tb]], axis=1)
            w = jnp.concatenate([wo[q, pa].reshape(256, 768), wo[q, pb].reshape(256, 768)], axis=0)
            part_sum = jnp.dot(m, w, preferred_element_type=F32)
            if n > 0:
                part_sum += acc[q]
            if n < 3:
                acc[q] = part_sum
            else:
                res[q] = (part_sum * mod[8 + q][0:1]).astype(BF)
            return carry

        if n < 3:
            lax.fori_loop(0, 4, out_part, 0)
        else:
            for q in range(4):
                out_part(q, 0)
                out_copy(q).start()

    for q in range(4):
        out_copy(q).wait()
    for c in sent:
        c.wait_send()
    for c in kv_all:
        c.wait_send()
    for c in az.values():
        c.wait_send()


def on_device(latents, timestep, w_mod, w_qkv, w_out):
    half_freq = w_mod.shape[0] // 2
    freqs = jnp.exp(-math.log(10000.0) * jnp.arange(half_freq, dtype=F32) / half_freq)
    angles = timestep.astype(F32)[:, None] * freqs[None, :]
    embed = jnp.concatenate([jnp.cos(angles), jnp.sin(angles)], axis=1).astype(BF)
    anyspace = pl.BlockSpec(memory_space=pl.ANY)
    out = pl.pallas_call(
        kernel,
        out_shape=jax.ShapeDtypeStruct((128, 3072), BF),
        in_specs=[pl.BlockSpec(memory_space=pltpu.VMEM)] + [anyspace] * 4,
        out_specs=anyspace,
        scratch_shapes=[
            pltpu.VMEM((256, 9216), BF),
            pltpu.VMEM((12, 16, 768), F32),
            pltpu.VMEM((8, 128, 3072), BF),
            pltpu.VMEM((8, 128, 3072), BF),
            pltpu.VMEM((2, 4, 2, 192, 768), BF),
            pltpu.VMEM((4, 8, 2, 2, 4, 16, 768), BF),
            pltpu.VMEM((8, 3072), BF),
            pltpu.VMEM((8, 3072), BF),
            pltpu.VMEM((8, 128, 256), BF),
            pltpu.VMEM((16, 128, 512), BF),
            pltpu.VMEM((8, 128, 256), BF),
            pltpu.VMEM((8, 128, 256), BF),
            pltpu.VMEM((4, 128, 768), F32),
            pltpu.VMEM((4, 128, 768), BF),
            pltpu.SemaphoreType.DMA((COUNT,)),
            pltpu.SemaphoreType.DMA((COUNT,)),
            pltpu.SemaphoreType.DMA((5,)),
        ],
        compiler_params=pltpu.CompilerParams(
            collective_id=0, has_side_effects=True, vmem_limit_bytes=60 * 1024 * 1024,
        ),
        name="sublayer",
    )(embed, latents[0], w_mod, w_qkv[0], w_out[0])
    return out[None]


def solution(mesh):
    placed = (P("grp", "sp", None), P("grp"), P(), P("sp", "grp", None), P("sp", "grp", None))
    return jax.shard_map(
        on_device, mesh=mesh, in_specs=placed, out_specs=P("grp", "sp", None), check_vma=False
    )
```
